32 devices in a mesh: grp: 2 (over y), row: 4 (over x, core), col: 4 (over z).
Axes of the slice: x: 2, y: 2, z: 4, core: 2. Of those that a mesh axis runs over, the one named last changes fastest.
Arguments:
- sigma_anc: float32 [1536, 768], P(('grp', 'row'), 'col'), parts along dimension 0, may hold values from -3 to 23, as said below
- anc_factor: float32 [1536, 2, 512], P(('grp', 'row', 'col')), parts along dimension 0, may hold values from -0.625 to 0.625
- diag_inverse: float32 [4, 512, 512], P('grp', None, 'row'), parts along dimension 0, may hold values from -0.6 to 1.5, as said below
- pattern: int32 [2, 6], replicated, may hold values from 0 to 1, as said below
Outputs:
- sel_off: float32 [1536, 2, 512], P(('grp', 'row', 'col')), parts along dimension 0
- sel_diag: float32 [4, 512, 512], P('grp'), parts along dimension 0
The draws below stay inside these ranges and needn't reach their ends.
There are 2 independent parts, one for each index of `grp`. The reference program is written for one: setup_inputs(seed, part) draws one part's arguments, and reference() takes and returns one part's arrays. A program takes and returns all parts, laid end to end along the dimension named above; an argument that names none is the same for every part. Nothing has to cross between parts.
Inputs may be any that keep to these rules, and one draw needn't show every extreme that they name: `pattern`: each supernode's present row blocks are a run of consecutive blocks, wrapping around the end, of at least 0 blocks, at most 3, together with some scattered others. `sigma_anc`: symmetric and positive definite. `diag_inverse`: lower triangular, with diagonal entries between 0.5 and 1.5 and small entries below the diagonal.
All inputs are finite; a program needn't handle non-finite values.
Results may differ from the reference program's by a relative error of at most 0.00013.
Values sent between devices are 32-bit elements; how exact they have to be, the bound alone decides.
A program may use at most 64 MiB of HBM per device.

```python
import math
import jax
import jax.numpy as jnp
from jax import lax

WID = 512
SUPERS = 2
BLK = 128
R = 768
NBLK = 6


def draw_sigma_anc(key, part):
    key = jax.random.fold_in(key, 11)
    key_noise, key_diag = jax.random.split(key, 2)
    noise = jax.random.normal(key_noise, (R, R), jnp.float32)
    matrix = (noise + jnp.transpose(noise)) * (0.3 / math.sqrt(R))
    diagonal = jax.random.uniform(key_diag, (R,), jnp.float32, 1.0, 2.0)
    matrix = matrix + jnp.diag(diagonal)
    return matrix


def draw_diag_inverse(key, part):
    key = jax.random.fold_in(key, 23)
    key_noise, key_diag = jax.random.split(key, 2)
    noise = jax.random.normal(key_noise, (SUPERS, WID, WID), jnp.float32) * (0.5 / math.sqrt(WID))
    lower = jnp.tril(noise, -1)
    diagonal = jax.random.uniform(key_diag, (SUPERS, WID), jnp.float32, 0.5, 1.5)
    identity = jnp.eye(WID, dtype=jnp.float32)
    return lower + diagonal[:, :, None] * identity[None, :, :]


def draw_pattern(key, part):
    key = jax.random.fold_in(key, 37)
    key_start, key_length, key_extra = jax.random.split(key, 3)
    first_block = jax.random.randint(key_start, (SUPERS, 1), 0, NBLK)
    run_length = jax.random.randint(key_length, (SUPERS, 1), max(1, NBLK // 8), NBLK // 2 + 1)
    positions = jnp.arange(NBLK, dtype=jnp.int32)[None, :]
    inside = (positions - first_block) % NBLK < run_length
    scattered = jax.random.randint(key_extra, (SUPERS, NBLK), 0, 8) == 0
    return jnp.where(inside | scattered, 1, 0).astype(jnp.int32)


def levels(stream_key, shape, cuts, smallest, top_value):
    gain = 1.0
    for position, blocks in cuts:
        heights = jax.random.uniform(jax.random.fold_in(jax.random.fold_in(stream_key, 6), position), (blocks,), jnp.float32, smallest / len(cuts), top_value / len(cuts))
        gain = gain * jnp.repeat(jnp.exp(heights), shape[position] // blocks).reshape((-1,) + (1,) * (len(shape) - 1 - position))
    return gain


def scatter_about(own_key, shape, width, bound, cuts=(), held_as=jnp.bfloat16):
    result = jax.random.normal(own_key, shape, jnp.float32) * width
    if len(cuts) > 0:
        result = levels(own_key, shape, cuts, -0.22, 0.18) * result
    return jnp.clip(result, min=-bound, max=bound).astype(held_as)


def setup_inputs(seed: int = 0, part: int = 0) -> dict:
    keys = jax.random.split(jax.random.key(seed), 5)
    part_keys = jax.random.split(jax.random.fold_in(keys[4], part), 5)
    return {
        "sigma_anc": draw_sigma_anc(jax.random.fold_in(jax.random.fold_in(keys[4], part), 71), part),
        "anc_factor": scatter_about(part_keys[1], (R, SUPERS, WID), (R // 8) ** -0.5, 0.625, ((0, 16),), jnp.float32),
        "diag_inverse": draw_diag_inverse(jax.random.fold_in(jax.random.fold_in(keys[4], part), 71), part),
        "pattern": draw_pattern(jax.random.fold_in(keys[4], 71), part),
    }


def reference(sigma_anc, anc_factor, diag_inverse, pattern):
    precise = lax.Precision.HIGHEST
    row_mask = jnp.repeat(pattern.astype(jnp.float32), BLK, axis=1)
    mask_rows = jnp.transpose(row_mask)[:, :, None]
    scaled = jnp.einsum("rsk,skj->rsj", anc_factor, diag_inverse, precision=precise) * mask_rows
    flattened = scaled.reshape(R, SUPERS * WID)
    product = jnp.dot(sigma_anc, flattened, precision=precise, preferred_element_type=jnp.float32)
    sel_off = -(product.reshape(R, SUPERS, WID) * mask_rows)
    first_term = jnp.einsum("skj,skl->sjl", diag_inverse, diag_inverse, precision=precise)
    second_term = jnp.einsum("rsj,rsl->sjl", scaled, sel_off, precision=precise)
    sel_diag = first_term - second_term
    return sel_off, sel_diag
```

```python
import functools

import jax
import jax.numpy as jnp
from jax import lax
from jax.experimental import pallas as pl
from jax.experimental.pallas import tpu as pltpu
from jax.sharding import PartitionSpec as P

LANES = 128
SUBLANES = 8


def split(x):
    high = x.astype(jnp.bfloat16)
    low = (x - high.astype(jnp.float32)).astype(jnp.bfloat16)
    return high, low


def dot3(a, b, contract=((1,), (0,))):
    (ah, al), (bh, bl) = a, b
    f = lambda u, v: lax.dot_general(u, v, (contract, ((), ())), preferred_element_type=jnp.float32)
    return f(ah, bh) + (f(ah, bl) + f(al, bh))


def fused_kernel(
    n_r, n_c, supers, width, rows_dev, block_size,
    sig_ref, a_ref, d_ref, pat_ref,
    off_ref, diag_ref,
    ag, ta, dfull, pbuf, rbuf, sbuf, rbuf2, left, right, goth, gown, grecv, hx, hrecv, zs, zrecv, res, tout, toff,
    send_sems, s_ag, s_ta, s_d, s_p, s_p2, s_g, s_h, s_z, s_zag, s_xag, s_sib, s_off, local_sems,
):
    r = lax.axis_index("row")
    c = lax.axis_index("col")
    n_x = n_r // 2
    x = r // 2
    k = r % 2
    sib = 2 * x + 1 - k
    piece = width // n_r
    nb = width // LANES
    half_rows = nb * (nb + 1) // 2 * LANES
    q = half_rows // (n_x * n_c)
    share = width // (n_r * n_c)
    block_rows = rows_dev * n_c
    sends = []

    def rcopy(src, dst, rsem, row, col):
        cp = pltpu.make_async_remote_copy(
            src_ref=src, dst_ref=dst, send_sem=send_sems.at[len(sends)], recv_sem=rsem,
            device_id={"row": row, "col": col}, device_id_type=pl.DeviceIdType.MESH,
        )
        cp.start()
        sends.append(cp)

    def wait_recv(dst, rsem):
        pltpu.make_async_copy(dst, dst, rsem).wait()

    barrier = pltpu.get_barrier_semaphore()
    sig = lambda row, col: pl.semaphore_signal(
        barrier, inc=1, device_id={"row": row, "col": col}, device_id_type=pl.DeviceIdType.MESH
    )
    for dc in range(1, n_c):
        sig(r, (c + dc) % n_c)
    sig(sib, c)
    for dx in range(1, n_x):
        sig(2 * ((x + dx) % n_x) + k, c)

    @pl.when(r != c)
    def _():
        sig(c, r)
        pl.semaphore_wait(barrier, n_c + n_x)

    @pl.when(r == c)
    def _():
        pl.semaphore_wait(barrier, n_c + n_x - 1)

    for dc in range(1, n_c):
        rcopy(a_ref, ag.at[c], s_ag.at[c], r, (c + dc) % n_c)
    d_slice = lambda ref, rr: ref.at[:, pl.ds(rr * piece, width - rr * piece), pl.ds(rr * piece, piece)]
    d_src = lambda rr: d_ref.at[:, pl.ds(rr * piece, width - rr * piece), :]

    def d_copy(src, rr, slot, row):
        return pltpu.make_async_remote_copy(
            src_ref=src, dst_ref=d_slice(dfull, rr), send_sem=send_sems.at[slot], recv_sem=s_d.at[rr],
            device_id={"row": row, "col": c}, device_id_type=pl.DeviceIdType.MESH,
        )

    n_fixed = 64
    for rr in range(n_r):
        @pl.when(r == rr)
        def _():
            for dx in range(1, n_x):
                d_copy(d_src(rr), rr, n_fixed + dx, 2 * ((x + dx) % n_x) + k).start()
            d_copy(d_src(rr), rr, n_fixed, sib).start()
            pltpu.make_async_copy(d_src(rr), d_slice(dfull, rr), local_sems.at[0]).start()
    own_copy = pltpu.make_async_copy(a_ref, ag.at[c], local_sems.at[1])
    own_copy.start()

    def ta_copy():
        return pltpu.make_async_remote_copy(
            src_ref=a_ref, dst_ref=ta, send_sem=send_sems.at[n_fixed - 1], recv_sem=s_ta.at[0],
            device_id={"row": c, "col": r}, device_id_type=pl.DeviceIdType.MESH,
        )

    ta_local = lambda: pltpu.make_async_copy(a_ref, ta, s_ta.at[0])

    @pl.when(r != c)
    def _():
        ta_copy().start()

    @pl.when(r == c)
    def _():
        ta_local().start()

    for rr in range(1, n_r):
        dfull[:, 0 : rr * piece, rr * piece : (rr + 1) * piece] = jnp.zeros((supers, rr * piece, piece), jnp.float32)

    def mask_of(first, rows, s):
        row = first + lax.broadcasted_iota(jnp.int32, (rows, 1), 0)
        m = jnp.zeros((rows, 1), jnp.float32)
        for b in range(pat_ref.shape[1]):
            inside = (row >= b * block_size) & (row < (b + 1) * block_size)
            m = jnp.where(inside, pat_ref[s, b].astype(jnp.float32), m)
        return m

    sigma_t = split(jnp.transpose(sig_ref[...]))

    for rr in range(n_r):
        @pl.when((rr % 2 == k) & (rr // 2 != x))
        def _():
            wait_recv(d_slice(dfull, rr), s_d.at[rr])
            d_copy(d_slice(dfull, rr), rr, n_fixed + n_x + rr // 2, sib).start()

    own_copy.wait()
    for dc in range(1, n_c):
        j = (c + dc) % n_c
        wait_recv(ag.at[j], s_ag.at[j])

    for s in range(supers):
        cols = slice(s * width, (s + 1) * width)
        block = ag[:, :, cols].reshape(block_rows, width) * mask_of(r * block_rows, block_rows, s)
        part = dot3(sigma_t, split(block))
        pbuf[:, :, cols] = part.reshape(n_r, rows_dev, width)
    for i in range(n_x):
        xo = (x + 1 + i) % n_x
        rcopy(pbuf.at[2 * xo + 1 - k], rbuf.at[xo], s_p.at[xo], sib, c)

    for rr in range(n_r):
        @pl.when((rr % 2 != k))
        def _():
            wait_recv(d_slice(dfull, rr), s_d.at[rr])

        @pl.when(r == rr)
        def _():
            pltpu.make_async_copy(d_src(rr), d_slice(dfull, rr), local_sems.at[0]).wait()

    wait_recv(ta, s_ta.at[0])

    for i in range(n_x):
        xo = (x + 1 + i) % n_x
        wait_recv(rbuf.at[xo], s_p.at[xo])
        sbuf[xo] = pbuf[2 * xo + k] + rbuf[xo]
        if i < n_x - 1:
            rcopy(sbuf.at[xo], rbuf2.at[x], s_p2.at[x], 2 * xo + k, c)

    t_first = (c * n_c + r) * rows_dev
    own_first = (r * n_c + c) * share
    masks = [mask_of(t_first, rows_dev, s) for s in range(supers)]
    step = 2 * LANES

    def times_d(rows_value, s, store):
        for j in range(0, width, step):
            xs = split(rows_value[:, j:])
            ds = split(dfull[s, j:, j : j + step])
            store(j, dot3(xs, ds))

    for s in range(supers):
        def store_scaled(j, v):
            left[s, 0:rows_dev, j : j + step] = -v
        times_d(ta[:, s * width : (s + 1) * width] * masks[s], s, store_scaled)
        own = dfull[s, pl.ds(pl.multiple_of(own_first, SUBLANES), share), :]
        left[s, rows_dev:, :] = own
        right[s, rows_dev:, :] = own

    for dx in range(1, n_x):
        xo = (x + dx) % n_x
        wait_recv(rbuf2.at[xo], s_p2.at[xo])
    for s in range(supers):
        cols = slice(s * width, (s + 1) * width)
        y = sbuf[x, :, cols]
        for dx in range(1, n_x):
            y = y + rbuf2[(x + dx) % n_x, :, cols]
        def store_off(j, v):
            right[s, 0:rows_dev, j : j + step] = v
            tout[:, s * width + j : s * width + j + step] = v
        times_d(y * (-masks[s]), s, store_off)

    def diag_part(s, dst):
        lh, ll = split(left[s])
        rh, rl = split(right[s])
        b = 0
        for i in range(nb):
            li = slice(i * LANES, (i + 1) * LANES)
            v = dot3((lh[:, li], ll[:, li]), (rh[:, : (i + 1) * LANES], rl[:, : (i + 1) * LANES]), ((0,), (0,)))
            for j in range(i + 1):
                dst[b * LANES : (b + 1) * LANES, :] = v[:, j * LANES : (j + 1) * LANES]
                b += 1

    diag_part(1 - k, goth)
    rcopy(goth, grecv, s_g.at[0], sib, c)

    def off_copy():
        return pltpu.make_async_remote_copy(
            src_ref=tout, dst_ref=toff, send_sem=send_sems.at[n_fixed - 2], recv_sem=s_off.at[0],
            device_id={"row": c, "col": r}, device_id_type=pl.DeviceIdType.MESH,
        )

    off_local = lambda: pltpu.make_async_copy(tout, toff, s_off.at[0])

    diag_part(k, gown)
    wait_recv(grecv, s_g.at[0])

    rows_at = lambda xo, j: pl.ds(pl.multiple_of((xo * n_c + j) * q, SUBLANES), q)
    for i in range(n_c):
        j = (c + 1 + i) % n_c
        for dx in range(1, n_x):
            xo = (x + dx) % n_x
            at = rows_at(xo, j)
            hx[at, :] = gown[at, :] + grecv[at, :]
            rcopy(hx.at[at, :], hrecv.at[x, j], s_h.at[x * n_c + j], 2 * xo + k, c)
    for i in range(n_c):
        j = (c + 1 + i) % n_c
        at = rows_at(x, j)
        v = gown[at, :] + grecv[at, :]
        for dx in range(1, n_x):
            xo = (x + dx) % n_x
            wait_recv(hrecv.at[xo, j], s_h.at[xo * n_c + j])
            v = v + hrecv[xo, j]
        zs[j] = v
        if i < n_c - 1:
            rcopy(zs.at[j], zrecv.at[c], s_z.at[c], r, j)

    @pl.when(r != c)
    def _():
        off_copy().start()

    @pl.when(r == c)
    def _():
        off_local().start()

    total = zs[c]
    for dc in range(1, n_c):
        j = (c + dc) % n_c
        wait_recv(zrecv.at[j], s_z.at[j])
        total = total + zrecv[j]
    mine = res.at[k, rows_at(x, c), :]
    res[k, rows_at(x, c), :] = total

    for dc in range(1, n_c):
        rcopy(mine, mine, s_zag.at[c], r, (c + dc) % n_c)
    def pass_on(j):
        chunk = res.at[k, rows_at(x, j), :]
        for dx in range(1, n_x):
            rcopy(chunk, chunk, s_xag.at[x * n_c + j], 2 * ((x + dx) % n_x) + k, c)
        rcopy(chunk, chunk, s_sib.at[x * n_c + j], sib, c)
    pass_on(c)
    for dc in range(1, n_c):
        j = (c + dc) % n_c
        wait_recv(res.at[k, rows_at(x, j), :], s_zag.at[j])
        pass_on(j)
    for dc in range(n_c):
        j = (c + dc) % n_c
        for dx in range(1, n_x):
            xo = (x + dx) % n_x
            chunk = res.at[k, rows_at(xo, j), :]
            wait_recv(chunk, s_xag.at[xo * n_c + j])
            rcopy(chunk, chunk, s_sib.at[xo * n_c + j], sib, c)

    wait_recv(toff, s_off.at[0])
    off_ref[...] = toff[...]

    def expand(s):
        b = 0
        for i in range(nb):
            for j in range(i + 1):
                v = res[s, b * LANES : (b + 1) * LANES, :]
                diag_ref[s, i * LANES : (i + 1) * LANES, j * LANES : (j + 1) * LANES] = v
                if j < i:
                    diag_ref[s, j * LANES : (j + 1) * LANES, i * LANES : (i + 1) * LANES] = jnp.transpose(v)
                b += 1

    expand(k)
    for xo in range(n_x):
        for j in range(n_c):
            wait_recv(res.at[1 - k, rows_at(xo, j), :], s_sib.at[xo * n_c + j])
    expand(1 - k)

    for cp in sends:
        cp.wait_send()
    for rr in range(n_r):
        @pl.when(r == rr)
        def _():
            for dx in range(1, n_x):
                d_copy(d_src(rr), rr, n_fixed + dx, 2 * ((x + dx) % n_x) + k).wait_send()
            d_copy(d_src(rr), rr, n_fixed, sib).wait_send()

        @pl.when((rr % 2 == k) & (rr // 2 != x))
        def _():
            d_copy(d_slice(dfull, rr), rr, n_fixed + n_x + rr // 2, sib).wait_send()

    @pl.when(r != c)
    def _():
        ta_copy().wait_send()
        off_copy().wait_send()


def fused_body(sigma_anc, anc_factor, diag_inverse, pattern):
    rows_dev, supers, width = anc_factor.shape
    n_r = lax.axis_size("row")
    n_c = lax.axis_size("col")
    n_x = n_r // 2
    total_rows = rows_dev * n_r * n_c
    flat = supers * width
    nb = width // LANES
    half_rows = nb * (nb + 1) // 2 * LANES
    q = half_rows // (n_x * n_c)
    share = width // (n_r * n_c)
    f32 = lambda *shape: pltpu.VMEM(shape, jnp.float32)
    dma = lambda n: pltpu.SemaphoreType.DMA((n,))
    vm = pl.BlockSpec(memory_space=pltpu.VMEM)
    off, diag = pl.pallas_call(
        functools.partial(fused_kernel, n_r, n_c, supers, width, rows_dev, total_rows // pattern.shape[1]),
        out_shape=(
            jax.ShapeDtypeStruct((rows_dev, flat), jnp.float32),
            jax.ShapeDtypeStruct((supers, width, width), jnp.float32),
        ),
        in_specs=[vm, vm, vm, pl.BlockSpec(memory_space=pltpu.SMEM)],
        out_specs=(vm, vm),
        scratch_shapes=[
            f32(n_c, rows_dev, flat),
            f32(rows_dev, flat),
            f32(supers, width, width),
            f32(n_r, rows_dev, flat),
            f32(n_x, rows_dev, flat),
            f32(n_x, rows_dev, flat),
            f32(n_x, rows_dev, flat),
            f32(supers, rows_dev + share, width),
            f32(supers, rows_dev + share, width),
            f32(half_rows, LANES),
            f32(half_rows, LANES),
            f32(half_rows, LANES),
            f32(half_rows, LANES),
            f32(n_x, n_c, q, LANES),
            f32(n_c, q, LANES),
            f32(n_c, q, LANES),
            f32(supers, half_rows, LANES),
            f32(rows_dev, flat),
            f32(rows_dev, flat),
            dma(64 + 2 * n_x),
            dma(n_c), dma(1), dma(n_r), dma(n_x), dma(n_x), dma(1), dma(n_x * n_c), dma(n_c), dma(n_c),
            dma(n_x * n_c), dma(n_x * n_c), dma(1), dma(2),
        ],
        compiler_params=pltpu.CompilerParams(
            collective_id=0, has_side_effects=True, vmem_limit_bytes=56 * 1024 * 1024
        ),
    )(sigma_anc, anc_factor.reshape(rows_dev, flat), diag_inverse, pattern)
    return off.reshape(anc_factor.shape), diag


def fits(sigma_anc, anc_factor, diag_inverse):
    rows_dev, supers, width = anc_factor.shape
    n_r = lax.axis_size("row")
    n_c = lax.axis_size("col")
    nb = width // LANES
    chunks = (n_r // 2) * n_c * SUBLANES
    return (
        n_r == n_c
        and n_r % 2 == 0
        and supers == 2
        and sigma_anc.shape[0] == sigma_anc.shape[1]
        and diag_inverse.shape[2] % LANES == 0
        and width % (2 * LANES) == 0
        and rows_dev % SUBLANES == 0
        and width % (n_r * n_c * SUBLANES) == 0
        and (nb * (nb + 1) // 2 * LANES) % chunks == 0
    )


def plain_body(sigma_anc, anc_factor, diag_inverse, pattern):
    precise = lax.Precision.HIGHEST
    rows_dev, supers, super_width = anc_factor.shape
    row_count = lax.axis_size("row")
    col_count = lax.axis_size("col")
    position = lax.axis_index("row") * col_count + lax.axis_index("col")
    total_rows = rows_dev * row_count * col_count
    block_size = total_rows // pattern.shape[1]
    flat_mask = jnp.repeat(pattern.astype(jnp.float32), block_size, axis=1)
    own_mask = jnp.transpose(lax.dynamic_slice_in_dim(flat_mask, position * rows_dev, rows_dev, 1))[
        :, :, None
    ]
    device_total = row_count * col_count
    share = -(-super_width // device_total)
    masked_factor = anc_factor * own_mask
    flattened = masked_factor.reshape(rows_dev, -1)
    gathered = lax.all_gather(flattened, "row", axis=0, tiled=True)
    stacked = gathered.reshape(row_count, rows_dev, flattened.shape[1])
    turned = lax.all_to_all(stacked, "col", split_axis=0, concat_axis=1, tiled=True)
    column_block = turned.reshape(row_count * rows_dev, flattened.shape[1])
    summed_rows = lax.psum_scatter(
        jnp.dot(sigma_anc, column_block, precision=precise, preferred_element_type=jnp.float32),
        "col",
        scatter_dimension=0,
        tiled=True,
    )
    off_factor = -(summed_rows.reshape(masked_factor.shape) * own_mask)
    both_rows = jnp.concatenate([masked_factor, off_factor], axis=0)
    column_piece = lax.all_gather(diag_inverse, "row", axis=2, tiled=True)
    product = jnp.einsum("rsk,skj->rsj", both_rows, column_piece, precision=precise)
    own_rows = lax.dynamic_slice_in_dim(column_piece, position * share, share, 1)
    scaled = product[:rows_dev]
    sel_off = product[rows_dev:]
    diag_term = jnp.einsum("skj,skl->sjl", own_rows, own_rows, precision=precise)
    partial_value = diag_term - jnp.einsum("rsj,rsl->sjl", scaled, sel_off, precision=precise)
    sel_diag = lax.psum(partial_value, ("row", "col"))
    return (sel_off, sel_diag)


def body(sigma_anc, anc_factor, diag_inverse, pattern):
    run = fused_body if fits(sigma_anc, anc_factor, diag_inverse) else plain_body
    return run(sigma_anc, anc_factor, diag_inverse, pattern)


def solution(mesh):
    return jax.shard_map(
        body,
        mesh=mesh,
        in_specs=(
            P(("grp", "row"), "col"),
            P(("grp", "row", "col"), None, None),
            P("grp", None, "row"),
            P(),
        ),
        out_specs=(P(("grp", "row", "col"), None, None), P("grp", None, None)),
        check_vma=False,
    )
```

```python
import functools

import jax
import jax.numpy as jnp
from jax import lax
from jax.experimental import pallas as pl
from jax.experimental.pallas import tpu as pltpu
from jax.sharding import PartitionSpec as P

LANES = 128
SUBLANES = 8


def split(x):
    high = x.astype(jnp.bfloat16)
    low = (x - high.astype(jnp.float32)).astype(jnp.bfloat16)
    return high, low


def dot3(a, b, contract=((1,), (0,))):
    (ah, al), (bh, bl) = a, b
    f = lambda u, v: lax.dot_general(u, v, (contract, ((), ())), preferred_element_type=jnp.float32)
    return f(ah, bh) + (f(ah, bl) + f(al, bh))


def fused_kernel(
    n_r, n_c, supers, width, rows_dev, block_size,
    sig_ref, a_ref, d_ref, pat_ref,
    off_ref, diag_ref,
    ag, sig_t, sq, dfull, pbuf, rbuf, sbuf, rbuf2, left, right, goth, gown, grecv, hx, hrecv, zs, zrecv, res,
    send_sems, s_ag, s_sq, s_d, s_p, s_p2, s_g, s_h, s_z, s_zag, s_xag, s_sib, local_sems,
):
    r = lax.axis_index("row")
    c = lax.axis_index("col")
    n_x = n_r // 2
    x = r // 2
    k = r % 2
    sib = 2 * x + 1 - k
    piece = width // n_r
    nb = width // LANES
    half_rows = nb * (nb + 1) // 2 * LANES
    q = half_rows // (n_x * n_c)
    share = width // (n_r * n_c)
    block_rows = rows_dev * n_c
    sends = []

    def rcopy(src, dst, rsem, row, col):
        cp = pltpu.make_async_remote_copy(
            src_ref=src, dst_ref=dst, send_sem=send_sems.at[len(sends)], recv_sem=rsem,
            device_id={"row": row, "col": col}, device_id_type=pl.DeviceIdType.MESH,
        )
        cp.start()
        sends.append(cp)

    def wait_recv(dst, rsem):
        pltpu.make_async_copy(dst, dst, rsem).wait()

    barrier = pltpu.get_barrier_semaphore()
    sig = lambda row, col: pl.semaphore_signal(
        barrier, inc=1, device_id={"row": row, "col": col}, device_id_type=pl.DeviceIdType.MESH
    )
    for dc in range(1, n_c):
        sig(r, (c + dc) % n_c)
    sig(sib, c)
    for dx in range(1, n_x):
        sig(2 * ((x + dx) % n_x) + k, c)

    pl.semaphore_wait(barrier, n_c + n_x - 1)

    n_line = 70
    def line_copy(src, j, d, to):
        slot = n_line + 2 * d + (1 if to > 0 else 0)
        return pltpu.make_async_remote_copy(
            src_ref=src, dst_ref=ag.at[j], send_sem=send_sems.at[slot], recv_sem=s_ag.at[j],
            device_id={"row": r, "col": (c + to + n_c) % n_c}, device_id_type=pl.DeviceIdType.MESH,
        )

    def line(d, to, f):
        for cc in range(n_c):
            j = cc - to * d
            if 0 <= j < n_c:
                @pl.when(c == cc)
                def _():
                    f(j, 0 <= cc + to < n_c)

    def start_own(j, onward, to):
        if onward:
            line_copy(a_ref, j, 0, to).start()

    for to in (1, -1):
        line(0, to, functools.partial(start_own, to=to))
    d_slice = lambda ref, rr: ref.at[:, pl.ds(rr * piece, width - rr * piece), pl.ds(rr * piece, piece)]
    d_src = lambda rr: d_ref.at[:, pl.ds(rr * piece, width - rr * piece), :]

    def d_copy(src, rr, slot, row):
        return pltpu.make_async_remote_copy(
            src_ref=src, dst_ref=d_slice(dfull, rr), send_sem=send_sems.at[slot], recv_sem=s_d.at[rr],
            device_id={"row": row, "col": c}, device_id_type=pl.DeviceIdType.MESH,
        )

    n_fixed = 64
    for rr in range(n_r):
        @pl.when(r == rr)
        def _():
            for dx in range(1, n_x):
                d_copy(d_src(rr), rr, n_fixed + dx, 2 * ((x + dx) % n_x) + k).start()
            d_copy(d_src(rr), rr, n_fixed, sib).start()
            pltpu.make_async_copy(d_src(rr), d_slice(dfull, rr), local_sems.at[0]).start()
    own_copy = pltpu.make_async_copy(a_ref, ag.at[c], local_sems.at[1])
    own_copy.start()

    sig_t[...] = jnp.transpose(sig_ref[...])
    sig_rows = lambda j: pl.ds(pl.multiple_of(j * rows_dev, SUBLANES), rows_dev)
    for dc in range(1, n_c):
        j = (c + dc) % n_c
        rcopy(sig_t.at[sig_rows(j), :], sq.at[c], s_sq.at[c], r, j)
    sq[c] = sig_t[sig_rows(c), :]

    for rr in range(1, n_r):
        dfull[:, 0 : rr * piece, rr * piece : (rr + 1) * piece] = jnp.zeros((supers, rr * piece, piece), jnp.float32)

    def mask_of(first, rows, s):
        row = first + lax.broadcasted_iota(jnp.int32, (rows, 1), 0)
        m = jnp.zeros((rows, 1), jnp.float32)
        for b in range(pat_ref.shape[1]):
            inside = (row >= b * block_size) & (row < (b + 1) * block_size)
            m = jnp.where(inside, pat_ref[s, b].astype(jnp.float32), m)
        return m

    def pass_line(j, onward, to, d):
        wait_recv(ag.at[j], s_ag.at[j])
        if onward:
            line_copy(ag.at[j], j, d, to).start()

    for d in range(1, n_c):
        for to in (1, -1):
            line(d, to, functools.partial(pass_line, to=to, d=d))

    for rr in range(n_r):
        @pl.when((rr % 2 == k) & (rr // 2 != x))
        def _():
            wait_recv(d_slice(dfull, rr), s_d.at[rr])
            d_copy(d_slice(dfull, rr), rr, n_fixed + n_x + rr // 2, sib).start()

    own_copy.wait()
    for dc in range(1, n_c):
        j = (c + dc) % n_c
        wait_recv(sq.at[j], s_sq.at[j])
    sigma_rows = split(sq[...].reshape(n_r * rows_dev, block_rows))

    for s in range(supers):
        cols = slice(s * width, (s + 1) * width)
        block = ag[:, :, cols].reshape(block_rows, width) * mask_of(r * block_rows, block_rows, s)
        part = dot3(sigma_rows, split(block))
        pbuf[:, :, cols] = part.reshape(n_r, rows_dev, width)
    for i in range(n_x):
        xo = (x + 1 + i) % n_x
        rcopy(pbuf.at[2 * xo + 1 - k], rbuf.at[xo], s_p.at[xo], sib, c)

    for rr in range(n_r):
        @pl.when((rr % 2 != k))
        def _():
            wait_recv(d_slice(dfull, rr), s_d.at[rr])

        @pl.when(r == rr)
        def _():
            pltpu.make_async_copy(d_src(rr), d_slice(dfull, rr), local_sems.at[0]).wait()

    for i in range(n_x):
        xo = (x + 1 + i) % n_x
        wait_recv(rbuf.at[xo], s_p.at[xo])
        sbuf[xo] = pbuf[2 * xo + k] + rbuf[xo]
        if i < n_x - 1:
            rcopy(sbuf.at[xo], rbuf2.at[x], s_p2.at[x], 2 * xo + k, c)

    t_first = (r * n_c + c) * rows_dev
    own_first = (r * n_c + c) * share
    masks = [mask_of(t_first, rows_dev, s) for s in range(supers)]
    step = 2 * LANES

    def times_d(rows_value, s, store):
        for j in range(0, width, step):
            xs = split(rows_value[:, j:])
            ds = split(dfull[s, j:, j : j + step])
            store(j, dot3(xs, ds))

    for s in range(supers):
        def store_scaled(j, v):
            left[s, 0:rows_dev, j : j + step] = -v
        times_d(a_ref[:, s * width : (s + 1) * width] * masks[s], s, store_scaled)
        own = dfull[s, pl.ds(pl.multiple_of(own_first, SUBLANES), share), :]
        left[s, rows_dev:, :] = own
        right[s, rows_dev:, :] = own

    for dx in range(1, n_x):
        xo = (x + dx) % n_x
        wait_recv(rbuf2.at[xo], s_p2.at[xo])
    for s in range(supers):
        cols = slice(s * width, (s + 1) * width)
        y = sbuf[x, :, cols]
        for dx in range(1, n_x):
            y = y + rbuf2[(x + dx) % n_x, :, cols]
        def store_off(j, v):
            right[s, 0:rows_dev, j : j + step] = v
            off_ref[:, s * width + j : s * width + j + step] = v
        times_d(y * (-masks[s]), s, store_off)

    def diag_part(s, dst):
        lh, ll = split(left[s])
        rh, rl = split(right[s])
        b = 0
        for i in range(nb):
            li = slice(i * LANES, (i + 1) * LANES)
            v = dot3((lh[:, li], ll[:, li]), (rh[:, : (i + 1) * LANES], rl[:, : (i + 1) * LANES]), ((0,), (0,)))
            for j in range(i + 1):
                dst[b * LANES : (b + 1) * LANES, :] = v[:, j * LANES : (j + 1) * LANES]
                b += 1

    diag_part(1 - k, goth)
    rcopy(goth, grecv, s_g.at[0], sib, c)

    diag_part(k, gown)
    wait_recv(grecv, s_g.at[0])

    rows_at = lambda xo, j: pl.ds(pl.multiple_of((xo * n_c + j) * q, SUBLANES), q)
    for i in range(n_c):
        j = (c + 1 + i) % n_c
        for dx in range(1, n_x):
            xo = (x + dx) % n_x
            at = rows_at(xo, j)
            hx[at, :] = gown[at, :] + grecv[at, :]
            rcopy(hx.at[at, :], hrecv.at[x, j], s_h.at[x * n_c + j], 2 * xo + k, c)
    for i in range(n_c):
        j = (c + 1 + i) % n_c
        at = rows_at(x, j)
        v = gown[at, :] + grecv[at, :]
        for dx in range(1, n_x):
            xo = (x + dx) % n_x
            wait_recv(hrecv.at[xo, j], s_h.at[xo * n_c + j])
            v = v + hrecv[xo, j]
        zs[j] = v
        if i < n_c - 1:
            rcopy(zs.at[j], zrecv.at[c], s_z.at[c], r, j)

    total = zs[c]
    for dc in range(1, n_c):
        j = (c + dc) % n_c
        wait_recv(zrecv.at[j], s_z.at[j])
        total = total + zrecv[j]
    mine = res.at[k, rows_at(x, c), :]
    res[k, rows_at(x, c), :] = total

    for dc in range(1, n_c):
        rcopy(mine, mine, s_zag.at[c], r, (c + dc) % n_c)
    def pass_on(j):
        chunk = res.at[k, rows_at(x, j), :]
        for dx in range(1, n_x):
            rcopy(chunk, chunk, s_xag.at[x * n_c + j], 2 * ((x + dx) % n_x) + k, c)
        rcopy(chunk, chunk, s_sib.at[x * n_c + j], sib, c)
    pass_on(c)
    for dc in range(1, n_c):
        j = (c + dc) % n_c
        wait_recv(res.at[k, rows_at(x, j), :], s_zag.at[j])
        pass_on(j)
    for dc in range(n_c):
        j = (c + dc) % n_c
        for dx in range(1, n_x):
            xo = (x + dx) % n_x
            chunk = res.at[k, rows_at(xo, j), :]
            wait_recv(chunk, s_xag.at[xo * n_c + j])
            rcopy(chunk, chunk, s_sib.at[xo * n_c + j], sib, c)

    def expand(s):
        b = 0
        for i in range(nb):
            for j in range(i + 1):
                v = res[s, b * LANES : (b + 1) * LANES, :]
                diag_ref[s, i * LANES : (i + 1) * LANES, j * LANES : (j + 1) * LANES] = v
                if j < i:
                    diag_ref[s, j * LANES : (j + 1) * LANES, i * LANES : (i + 1) * LANES] = jnp.transpose(v)
                b += 1

    expand(k)
    for xo in range(n_x):
        for j in range(n_c):
            wait_recv(res.at[1 - k, rows_at(xo, j), :], s_sib.at[xo * n_c + j])
    expand(1 - k)

    for cp in sends:
        cp.wait_send()
    for rr in range(n_r):
        @pl.when(r == rr)
        def _():
            for dx in range(1, n_x):
                d_copy(d_src(rr), rr, n_fixed + dx, 2 * ((x + dx) % n_x) + k).wait_send()
            d_copy(d_src(rr), rr, n_fixed, sib).wait_send()

        @pl.when((rr % 2 == k) & (rr // 2 != x))
        def _():
            d_copy(d_slice(dfull, rr), rr, n_fixed + n_x + rr // 2, sib).wait_send()

    def sent(j, onward, to, d):
        if onward:
            line_copy(a_ref, j, d, to).wait_send()

    for d in range(n_c):
        for to in (1, -1):
            line(d, to, functools.partial(sent, to=to, d=d))


def fused_body(sigma_anc, anc_factor, diag_inverse, pattern):
    rows_dev, supers, width = anc_factor.shape
    n_r = lax.axis_size("row")
    n_c = lax.axis_size("col")
    n_x = n_r // 2
    total_rows = rows_dev * n_r * n_c
    flat = supers * width
    nb = width // LANES
    half_rows = nb * (nb + 1) // 2 * LANES
    q = half_rows // (n_x * n_c)
    share = width // (n_r * n_c)
    f32 = lambda *shape: pltpu.VMEM(shape, jnp.float32)
    dma = lambda n: pltpu.SemaphoreType.DMA((n,))
    vm = pl.BlockSpec(memory_space=pltpu.VMEM)
    off, diag = pl.pallas_call(
        functools.partial(fused_kernel, n_r, n_c, supers, width, rows_dev, total_rows // pattern.shape[1]),
        out_shape=(
            jax.ShapeDtypeStruct((rows_dev, flat), jnp.float32),
            jax.ShapeDtypeStruct((supers, width, width), jnp.float32),
        ),
        in_specs=[vm, vm, vm, pl.BlockSpec(memory_space=pltpu.SMEM)],
        out_specs=(vm, vm),
        scratch_shapes=[
            f32(n_c, rows_dev, flat),
            f32(n_r * rows_dev, n_c * rows_dev),
            f32(n_c, rows_dev, n_c * rows_dev),
            f32(supers, width, width),
            f32(n_r, rows_dev, flat),
            f32(n_x, rows_dev, flat),
            f32(n_x, rows_dev, flat),
            f32(n_x, rows_dev, flat),
            f32(supers, rows_dev + share, width),
            f32(supers, rows_dev + share, width),
            f32(half_rows, LANES),
            f32(half_rows, LANES),
            f32(half_rows, LANES),
            f32(half_rows, LANES),
            f32(n_x, n_c, q, LANES),
            f32(n_c, q, LANES),
            f32(n_c, q, LANES),
            f32(supers, half_rows, LANES),
            dma(70 + 2 * n_c),
            dma(n_c), dma(n_c), dma(n_r), dma(n_x), dma(n_x), dma(1), dma(n_x * n_c), dma(n_c), dma(n_c),
            dma(n_x * n_c), dma(n_x * n_c), dma(2),
        ],
        compiler_params=pltpu.CompilerParams(
            collective_id=0, has_side_effects=True, vmem_limit_bytes=56 * 1024 * 1024
        ),
    )(sigma_anc, anc_factor.reshape(rows_dev, flat), diag_inverse, pattern)
    return off.reshape(anc_factor.shape), diag


def fits(sigma_anc, anc_factor, diag_inverse):
    rows_dev, supers, width = anc_factor.shape
    n_r = lax.axis_size("row")
    n_c = lax.axis_size("col")
    nb = width // LANES
    chunks = (n_r // 2) * n_c * SUBLANES
    return (
        n_r == n_c
        and n_r % 2 == 0
        and supers == 2
        and sigma_anc.shape[0] == sigma_anc.shape[1]
        and diag_inverse.shape[2] % LANES == 0
        and width % (2 * LANES) == 0
        and rows_dev % SUBLANES == 0
        and width % (n_r * n_c * SUBLANES) == 0
        and (nb * (nb + 1) // 2 * LANES) % chunks == 0
    )


def plain_body(sigma_anc, anc_factor, diag_inverse, pattern):
    precise = lax.Precision.HIGHEST
    rows_dev, supers, super_width = anc_factor.shape
    row_count = lax.axis_size("row")
    col_count = lax.axis_size("col")
    position = lax.axis_index("row") * col_count + lax.axis_index("col")
    total_rows = rows_dev * row_count * col_count
    block_size = total_rows // pattern.shape[1]
    flat_mask = jnp.repeat(pattern.astype(jnp.float32), block_size, axis=1)
    own_mask = jnp.transpose(lax.dynamic_slice_in_dim(flat_mask, position * rows_dev, rows_dev, 1))[
        :, :, None
    ]
    device_total = row_count * col_count
    share = -(-super_width // device_total)
    masked_factor = anc_factor * own_mask
    flattened = masked_factor.reshape(rows_dev, -1)
    gathered = lax.all_gather(flattened, "row", axis=0, tiled=True)
    stacked = gathered.reshape(row_count, rows_dev, flattened.shape[1])
    turned = lax.all_to_all(stacked, "col", split_axis=0, concat_axis=1, tiled=True)
    column_block = turned.reshape(row_count * rows_dev, flattened.shape[1])
    summed_rows = lax.psum_scatter(
        jnp.dot(sigma_anc, column_block, precision=precise, preferred_element_type=jnp.float32),
        "col",
        scatter_dimension=0,
        tiled=True,
    )
    off_factor = -(summed_rows.reshape(masked_factor.shape) * own_mask)
    both_rows = jnp.concatenate([masked_factor, off_factor], axis=0)
    column_piece = lax.all_gather(diag_inverse, "row", axis=2, tiled=True)
    product = jnp.einsum("rsk,skj->rsj", both_rows, column_piece, precision=precise)
    own_rows = lax.dynamic_slice_in_dim(column_piece, position * share, share, 1)
    scaled = product[:rows_dev]
    sel_off = product[rows_dev:]
    diag_term = jnp.einsum("skj,skl->sjl", own_rows, own_rows, precision=precise)
    partial_value = diag_term - jnp.einsum("rsj,rsl->sjl", scaled, sel_off, precision=precise)
    sel_diag = lax.psum(partial_value, ("row", "col"))
    return (sel_off, sel_diag)


def body(sigma_anc, anc_factor, diag_inverse, pattern):
    run = fused_body if fits(sigma_anc, anc_factor, diag_inverse) else plain_body
    return run(sigma_anc, anc_factor, diag_inverse, pattern)


def solution(mesh):
    return jax.shard_map(
        body,
        mesh=mesh,
        in_specs=(
            P(("grp", "row"), "col"),
            P(("grp", "row", "col"), None, None),
            P("grp", None, "row"),
            P(),
        ),
        out_specs=(P(("grp", "row", "col"), None, None), P("grp", None, None)),
        check_vma=False,
    )
```

```python
import functools

import jax
import jax.numpy as jnp
from jax import lax
from jax.experimental import pallas as pl
from jax.experimental.pallas import tpu as pltpu
from jax.sharding import PartitionSpec as P

LANES = 128
SUBLANES = 8


def split(x):
    high = x.astype(jnp.bfloat16)
    low = (x - high.astype(jnp.float32)).astype(jnp.bfloat16)
    return high, low


def dot3(a, b, contract=((1,), (0,))):
    (ah, al), (bh, bl) = a, b
    f = lambda u, v: lax.dot_general(u, v, (contract, ((), ())), preferred_element_type=jnp.float32)
    return f(ah, bh) + (f(ah, bl) + f(al, bh))


def fused_kernel(
    n_r, n_c, supers, width, rows_dev, block_size,
    sig_ref, a_ref, d_ref, pat_ref,
    off_ref, diag_ref,
    ag, sig_t, sq, dfull, pbuf, rbuf, sbuf, rbuf2, left, right, goth, gown, grecv, hx, hrecv, zs, zrecv, res,
    send_sems, s_ag, s_sq, s_d, s_p, s_p2, s_g, s_h, s_z, s_zag, s_xag, s_sib, local_sems,
):
    r = lax.axis_index("row")
    c = lax.axis_index("col")
    n_x = n_r // 2
    x = r // 2
    k = r % 2
    sib = 2 * x + 1 - k
    piece = width // n_r
    nb = width // LANES
    half_rows = nb * (nb + 1) // 2 * LANES
    q = half_rows // (n_x * n_c)
    share = width // (n_r * n_c)
    block_rows = rows_dev * n_c
    sends = []

    def rcopy(src, dst, rsem, row, col):
        cp = pltpu.make_async_remote_copy(
            src_ref=src, dst_ref=dst, send_sem=send_sems.at[len(sends)], recv_sem=rsem,
            device_id={"row": row, "col": col}, device_id_type=pl.DeviceIdType.MESH,
        )
        cp.start()
        sends.append(cp)

    def wait_recv(dst, rsem):
        pltpu.make_async_copy(dst, dst, rsem).wait()

    barrier = pltpu.get_barrier_semaphore()
    sig = lambda row, col: pl.semaphore_signal(
        barrier, inc=1, device_id={"row": row, "col": col}, device_id_type=pl.DeviceIdType.MESH
    )
    for dc in range(1, n_c):
        sig(r, (c + dc) % n_c)
    sig(sib, c)
    for dx in range(1, n_x):
        sig(2 * ((x + dx) % n_x) + k, c)

    pl.semaphore_wait(barrier, n_c + n_x - 1)

    n_line = 70
    part_of = lambda j, h: ag.at[j, :, pl.ds(h * width, width)]
    own_part = lambda h: a_ref.at[:, pl.ds(h * width, width)]

    def line_copy(src, j, d, to, h):
        slot = n_line + (2 * d + (1 if to > 0 else 0)) * supers + h
        return pltpu.make_async_remote_copy(
            src_ref=src, dst_ref=part_of(j, h), send_sem=send_sems.at[slot], recv_sem=s_ag.at[j * supers + h],
            device_id={"row": r, "col": (c + to + n_c) % n_c}, device_id_type=pl.DeviceIdType.MESH,
        )

    def line(d, to, f):
        for cc in range(n_c):
            j = cc - to * d
            if 0 <= j < n_c:
                @pl.when(c == cc)
                def _():
                    f(j, 0 <= cc + to < n_c)

    def start_own(j, onward, to, h):
        if onward:
            line_copy(own_part(h), j, 0, to, h).start()

    for h in range(supers):
        for to in (1, -1):
            line(0, to, functools.partial(start_own, to=to, h=h))
    d_slice = lambda ref, rr: ref.at[:, pl.ds(rr * piece, width - rr * piece), pl.ds(rr * piece, piece)]
    d_src = lambda rr: d_ref.at[:, pl.ds(rr * piece, width - rr * piece), :]

    def d_copy(src, rr, slot, row):
        return pltpu.make_async_remote_copy(
            src_ref=src, dst_ref=d_slice(dfull, rr), send_sem=send_sems.at[slot], recv_sem=s_d.at[rr],
            device_id={"row": row, "col": c}, device_id_type=pl.DeviceIdType.MESH,
        )

    n_fixed = 64
    for rr in range(n_r):
        @pl.when(r == rr)
        def _():
            for dx in range(1, n_x):
                d_copy(d_src(rr), rr, n_fixed + dx, 2 * ((x + dx) % n_x) + k).start()
            d_copy(d_src(rr), rr, n_fixed, sib).start()
            pltpu.make_async_copy(d_src(rr), d_slice(dfull, rr), local_sems.at[0]).start()
    own_copy = pltpu.make_async_copy(a_ref, ag.at[c], local_sems.at[1])
    own_copy.start()

    sig_t[...] = jnp.transpose(sig_ref[...])
    sig_rows = lambda j: pl.ds(pl.multiple_of(j * rows_dev, SUBLANES), rows_dev)
    for dc in range(1, n_c):
        j = (c + dc) % n_c
        rcopy(sig_t.at[sig_rows(j), :], sq.at[c], s_sq.at[c], r, j)
    sq[c] = sig_t[sig_rows(c), :]

    for rr in range(1, n_r):
        dfull[:, 0 : rr * piece, rr * piece : (rr + 1) * piece] = jnp.zeros((supers, rr * piece, piece), jnp.float32)

    def mask_of(first, rows, s):
        row = first + lax.broadcasted_iota(jnp.int32, (rows, 1), 0)
        m = jnp.zeros((rows, 1), jnp.float32)
        for b in range(pat_ref.shape[1]):
            inside = (row >= b * block_size) & (row < (b + 1) * block_size)
            m = jnp.where(inside, pat_ref[s, b].astype(jnp.float32), m)
        return m

    def pass_line(j, onward, to, d, h):
        wait_recv(part_of(j, h), s_ag.at[j * supers + h])
        if onward:
            line_copy(part_of(j, h), j, d, to, h).start()

    for d in range(1, n_c):
        for h in range(supers):
            for to in (1, -1):
                line(d, to, functools.partial(pass_line, to=to, d=d, h=h))

    for rr in range(n_r):
        @pl.when((rr % 2 == k) & (rr // 2 != x))
        def _():
            wait_recv(d_slice(dfull, rr), s_d.at[rr])
            d_copy(d_slice(dfull, rr), rr, n_fixed + n_x + rr // 2, sib).start()

    own_copy.wait()
    for dc in range(1, n_c):
        j = (c + dc) % n_c
        wait_recv(sq.at[j], s_sq.at[j])
    sigma_rows = split(sq[...].reshape(n_r * rows_dev, block_rows))

    for s in range(supers):
        cols = slice(s * width, (s + 1) * width)
        block = ag[:, :, cols].reshape(block_rows, width) * mask_of(r * block_rows, block_rows, s)
        part = dot3(sigma_rows, split(block))
        pbuf[:, :, cols] = part.reshape(n_r, rows_dev, width)
    for i in range(n_x):
        xo = (x + 1 + i) % n_x
        rcopy(pbuf.at[2 * xo + 1 - k], rbuf.at[xo], s_p.at[xo], sib, c)

    for rr in range(n_r):
        @pl.when((rr % 2 != k))
        def _():
            wait_recv(d_slice(dfull, rr), s_d.at[rr])

        @pl.when(r == rr)
        def _():
            pltpu.make_async_copy(d_src(rr), d_slice(dfull, rr), local_sems.at[0]).wait()

    for i in range(n_x):
        xo = (x + 1 + i) % n_x
        wait_recv(rbuf.at[xo], s_p.at[xo])
        sbuf[xo] = pbuf[2 * xo + k] + rbuf[xo]
        if i < n_x - 1:
            rcopy(sbuf.at[xo], rbuf2.at[x], s_p2.at[x], 2 * xo + k, c)

    t_first = (r * n_c + c) * rows_dev
    own_first = (r * n_c + c) * share
    masks = [mask_of(t_first, rows_dev, s) for s in range(supers)]
    step = 2 * LANES

    def times_d(rows_value, s, store):
        for j in range(0, width, step):
            xs = split(rows_value[:, j:])
            ds = split(dfull[s, j:, j : j + step])
            store(j, dot3(xs, ds))

    for s in range(supers):
        def store_scaled(j, v):
            left[s, 0:rows_dev, j : j + step] = -v
        times_d(a_ref[:, s * width : (s + 1) * width] * masks[s], s, store_scaled)
        own = dfull[s, pl.ds(pl.multiple_of(own_first, SUBLANES), share), :]
        left[s, rows_dev:, :] = own
        right[s, rows_dev:, :] = own

    for dx in range(1, n_x):
        xo = (x + dx) % n_x
        wait_recv(rbuf2.at[xo], s_p2.at[xo])
    for s in range(supers):
        cols = slice(s * width, (s + 1) * width)
        y = sbuf[x, :, cols]
        for dx in range(1, n_x):
            y = y + rbuf2[(x + dx) % n_x, :, cols]
        def store_off(j, v):
            right[s, 0:rows_dev, j : j + step] = v
            off_ref[:, s * width + j : s * width + j + step] = v
        times_d(y * (-masks[s]), s, store_off)

    def diag_part(s, dst):
        lh, ll = split(left[s])
        rh, rl = split(right[s])
        b = 0
        for i in range(nb):
            li = slice(i * LANES, (i + 1) * LANES)
            v = dot3((lh[:, li], ll[:, li]), (rh[:, : (i + 1) * LANES], rl[:, : (i + 1) * LANES]), ((0,), (0,)))
            for j in range(i + 1):
                dst[b * LANES : (b + 1) * LANES, :] = v[:, j * LANES : (j + 1) * LANES]
                b += 1

    diag_part(1 - k, goth)
    rcopy(goth, grecv, s_g.at[0], sib, c)

    diag_part(k, gown)
    wait_recv(grecv, s_g.at[0])

    rows_at = lambda xo, j: pl.ds(pl.multiple_of((xo * n_c + j) * q, SUBLANES), q)
    for i in range(n_c):
        j = (c + 1 + i) % n_c
        for dx in range(1, n_x):
            xo = (x + dx) % n_x
            at = rows_at(xo, j)
            hx[at, :] = gown[at, :] + grecv[at, :]
            rcopy(hx.at[at, :], hrecv.at[x, j], s_h.at[x * n_c + j], 2 * xo + k, c)
    for i in range(n_c):
        j = (c + 1 + i) % n_c
        at = rows_at(x, j)
        v = gown[at, :] + grecv[at, :]
        for dx in range(1, n_x):
            xo = (x + dx) % n_x
            wait_recv(hrecv.at[xo, j], s_h.at[xo * n_c + j])
            v = v + hrecv[xo, j]
        zs[j] = v
        if i < n_c - 1:
            rcopy(zs.at[j], zrecv.at[c], s_z.at[c], r, j)

    total = zs[c]
    for dc in range(1, n_c):
        j = (c + dc) % n_c
        wait_recv(zrecv.at[j], s_z.at[j])
        total = total + zrecv[j]
    mine = res.at[k, rows_at(x, c), :]
    res[k, rows_at(x, c), :] = total

    for dc in range(1, n_c):
        rcopy(mine, mine, s_zag.at[c], r, (c + dc) % n_c)
    def pass_on(j):
        chunk = res.at[k, rows_at(x, j), :]
        for dx in range(1, n_x):
            rcopy(chunk, chunk, s_xag.at[x * n_c + j], 2 * ((x + dx) % n_x) + k, c)
        rcopy(chunk, chunk, s_sib.at[x * n_c + j], sib, c)
    pass_on(c)
    for dc in range(1, n_c):
        j = (c + dc) % n_c
        wait_recv(res.at[k, rows_at(x, j), :], s_zag.at[j])
        pass_on(j)
    for dc in range(n_c):
        j = (c + dc) % n_c
        for dx in range(1, n_x):
            xo = (x + dx) % n_x
            chunk = res.at[k, rows_at(xo, j), :]
            wait_recv(chunk, s_xag.at[xo * n_c + j])
            rcopy(chunk, chunk, s_sib.at[xo * n_c + j], sib, c)

    def expand(s):
        b = 0
        for i in range(nb):
            for j in range(i + 1):
                v = res[s, b * LANES : (b + 1) * LANES, :]
                diag_ref[s, i * LANES : (i + 1) * LANES, j * LANES : (j + 1) * LANES] = v
                if j < i:
                    diag_ref[s, j * LANES : (j + 1) * LANES, i * LANES : (i + 1) * LANES] = jnp.transpose(v)
                b += 1

    expand(k)
    for xo in range(n_x):
        for j in range(n_c):
            wait_recv(res.at[1 - k, rows_at(xo, j), :], s_sib.at[xo * n_c + j])
    expand(1 - k)

    for cp in sends:
        cp.wait_send()
    for rr in range(n_r):
        @pl.when(r == rr)
        def _():
            for dx in range(1, n_x):
                d_copy(d_src(rr), rr, n_fixed + dx, 2 * ((x + dx) % n_x) + k).wait_send()
            d_copy(d_src(rr), rr, n_fixed, sib).wait_send()

        @pl.when((rr % 2 == k) & (rr // 2 != x))
        def _():
            d_copy(d_slice(dfull, rr), rr, n_fixed + n_x + rr // 2, sib).wait_send()

    def sent(j, onward, to, d, h):
        if onward:
            line_copy(own_part(h), j, d, to, h).wait_send()

    for d in range(n_c):
        for h in range(supers):
            for to in (1, -1):
                line(d, to, functools.partial(sent, to=to, d=d, h=h))


def fused_body(sigma_anc, anc_factor, diag_inverse, pattern):
    rows_dev, supers, width = anc_factor.shape
    n_r = lax.axis_size("row")
    n_c = lax.axis_size("col")
    n_x = n_r // 2
    total_rows = rows_dev * n_r * n_c
    flat = supers * width
    nb = width // LANES
    half_rows = nb * (nb + 1) // 2 * LANES
    q = half_rows // (n_x * n_c)
    share = width // (n_r * n_c)
    f32 = lambda *shape: pltpu.VMEM(shape, jnp.float32)
    dma = lambda n: pltpu.SemaphoreType.DMA((n,))
    vm = pl.BlockSpec(memory_space=pltpu.VMEM)
    off, diag = pl.pallas_call(
        functools.partial(fused_kernel, n_r, n_c, supers, width, rows_dev, total_rows // pattern.shape[1]),
        out_shape=(
            jax.ShapeDtypeStruct((rows_dev, flat), jnp.float32),
            jax.ShapeDtypeStruct((supers, width, width), jnp.float32),
        ),
        in_specs=[vm, vm, vm, pl.BlockSpec(memory_space=pltpu.SMEM)],
        out_specs=(vm, vm),
        scratch_shapes=[
            f32(n_c, rows_dev, flat),
            f32(n_r * rows_dev, n_c * rows_dev),
            f32(n_c, rows_dev, n_c * rows_dev),
            f32(supers, width, width),
            f32(n_r, rows_dev, flat),
            f32(n_x, rows_dev, flat),
            f32(n_x, rows_dev, flat),
            f32(n_x, rows_dev, flat),
            f32(supers, rows_dev + share, width),
            f32(supers, rows_dev + share, width),
            f32(half_rows, LANES),
            f32(half_rows, LANES),
            f32(half_rows, LANES),
            f32(half_rows, LANES),
            f32(n_x, n_c, q, LANES),
            f32(n_c, q, LANES),
            f32(n_c, q, LANES),
            f32(supers, half_rows, LANES),
            dma(70 + 2 * n_c * supers),
            dma(n_c * supers), dma(n_c), dma(n_r), dma(n_x), dma(n_x), dma(1), dma(n_x * n_c), dma(n_c), dma(n_c),
            dma(n_x * n_c), dma(n_x * n_c), dma(2),
        ],
        compiler_params=pltpu.CompilerParams(
            collective_id=0, has_side_effects=True, vmem_limit_bytes=56 * 1024 * 1024
        ),
    )(sigma_anc, anc_factor.reshape(rows_dev, flat), diag_inverse, pattern)
    return off.reshape(anc_factor.shape), diag


def fits(sigma_anc, anc_factor, diag_inverse):
    rows_dev, supers, width = anc_factor.shape
    n_r = lax.axis_size("row")
    n_c = lax.axis_size("col")
    nb = width // LANES
    chunks = (n_r // 2) * n_c * SUBLANES
    return (
        n_r == n_c
        and n_r % 2 == 0
        and supers == 2
        and sigma_anc.shape[0] == sigma_anc.shape[1]
        and diag_inverse.shape[2] % LANES == 0
        and width % (2 * LANES) == 0
        and rows_dev % SUBLANES == 0
        and width % (n_r * n_c * SUBLANES) == 0
        and (nb * (nb + 1) // 2 * LANES) % chunks == 0
    )


def plain_body(sigma_anc, anc_factor, diag_inverse, pattern):
    precise = lax.Precision.HIGHEST
    rows_dev, supers, super_width = anc_factor.shape
    row_count = lax.axis_size("row")
    col_count = lax.axis_size("col")
    position = lax.axis_index("row") * col_count + lax.axis_index("col")
    total_rows = rows_dev * row_count * col_count
    block_size = total_rows // pattern.shape[1]
    flat_mask = jnp.repeat(pattern.astype(jnp.float32), block_size, axis=1)
    own_mask = jnp.transpose(lax.dynamic_slice_in_dim(flat_mask, position * rows_dev, rows_dev, 1))[
        :, :, None
    ]
    device_total = row_count * col_count
    share = -(-super_width // device_total)
    masked_factor = anc_factor * own_mask
    flattened = masked_factor.reshape(rows_dev, -1)
    gathered = lax.all_gather(flattened, "row", axis=0, tiled=True)
    stacked = gathered.reshape(row_count, rows_dev, flattened.shape[1])
    turned = lax.all_to_all(stacked, "col", split_axis=0, concat_axis=1, tiled=True)
    column_block = turned.reshape(row_count * rows_dev, flattened.shape[1])
    summed_rows = lax.psum_scatter(
        jnp.dot(sigma_anc, column_block, precision=precise, preferred_element_type=jnp.float32),
        "col",
        scatter_dimension=0,
        tiled=True,
    )
    off_factor = -(summed_rows.reshape(masked_factor.shape) * own_mask)
    both_rows = jnp.concatenate([masked_factor, off_factor], axis=0)
    column_piece = lax.all_gather(diag_inverse, "row", axis=2, tiled=True)
    product = jnp.einsum("rsk,skj->rsj", both_rows, column_piece, precision=precise)
    own_rows = lax.dynamic_slice_in_dim(column_piece, position * share, share, 1)
    scaled = product[:rows_dev]
    sel_off = product[rows_dev:]
    diag_term = jnp.einsum("skj,skl->sjl", own_rows, own_rows, precision=precise)
    partial_value = diag_term - jnp.einsum("rsj,rsl->sjl", scaled, sel_off, precision=precise)
    sel_diag = lax.psum(partial_value, ("row", "col"))
    return (sel_off, sel_diag)


def body(sigma_anc, anc_factor, diag_inverse, pattern):
    run = fused_body if fits(sigma_anc, anc_factor, diag_inverse) else plain_body
    return run(sigma_anc, anc_factor, diag_inverse, pattern)


def solution(mesh):
    return jax.shard_map(
        body,
        mesh=mesh,
        in_specs=(
            P(("grp", "row"), "col"),
            P(("grp", "row", "col"), None, None),
            P("grp", None, "row"),
            P(),
        ),
        out_specs=(P(("grp", "row", "col"), None, None), P("grp", None, None)),
        check_vma=False,
    )
```
